32 devices in a mesh: pole: 2 (over y), leaf: 16 (over z, x, core).
Axes of the slice: x: 2, y: 2, z: 4, core: 2. Of those that a mesh axis runs over, the one named last changes fastest.
Arguments:
- root_frame: float32 [2048, 1024], P(('pole', 'leaf')), parts along dimension 0, may hold values from -2 to 8, as said below
- top_lhat: float32 [3072, 256], P(('pole', 'leaf')), parts along dimension 0, may hold values from -0.21875 to 0.21875
- top_dinv: float32 [1024, 256], P(('pole', 'leaf')), parts along dimension 0, may hold values from -2 to 8, as said below
- mid_lhat: float32 [32, 768, 256], P(('pole', 'leaf')), parts along dimension 0, may hold values from -0.21875 to 0.21875
- mid_dinv: float32 [32, 256, 256], P(('pole', 'leaf')), parts along dimension 0, may hold values from -2 to 8, as said below
- leaf_lhat: float32 [64, 768, 256], P(('pole', 'leaf')), parts along dimension 0, may hold values from -0.21875 to 0.21875
- leaf_dinv: float32 [64, 256, 256], P(('pole', 'leaf')), parts along dimension 0, may hold values from -2 to 8, as said below
- top_columns: int32 [2], replicated, may hold values from 128 to 256
- mid_columns: int32 [16], replicated, may hold values from 128 to 256
- leaf_columns: int32 [32], replicated, may hold values from 128 to 256
- top_pattern: int32 [2, 3], replicated, may hold values from 0 to 3, as said below
- mid_parent: int32 [16], replicated, may hold values from 0 to 1, as said below
- leaf_parent: int32 [32], replicated, may hold values from 0 to 15, as said below
- mid_pattern: int32 [16, 3], replicated, may hold values from 0 to 3, as said below
- leaf_pattern: int32 [32, 3], replicated, may hold values from 0 to 3, as said below
- leaf_live: int32 [16], replicated, may hold values from 1 to 2, as said below
Outputs:
- top_diagonal: float32 [1024, 256], P(('pole', 'leaf')), parts along dimension 0
- top_coupling: float32 [3072, 256], P(('pole', 'leaf')), parts along dimension 0
- mid_diagonal: float32 [32, 256, 256], P(('pole', 'leaf')), parts along dimension 0
- mid_coupling: float32 [32, 768, 256], P(('pole', 'leaf')), parts along dimension 0
- leaf_diagonal: float32 [64, 256, 256], P(('pole', 'leaf')), parts along dimension 0
- leaf_coupling: float32 [64, 768, 256], P(('pole', 'leaf')), parts along dimension 0
The draws below stay inside these ranges and needn't reach their ends.
There are 2 independent parts, one for each index of `pole`. The reference program is written for one: setup_inputs(seed, part) draws one part's arguments, and reference() takes and returns one part's arrays. A program takes and returns all parts, laid end to end along the dimension named above; an argument that names none is the same for every part. Nothing has to cross between parts.
Inputs may be any that keep to these rules, and one draw needn't show every extreme that they name: `root_frame`: Symmetric. `top_dinv`: each 256 x 256 block is symmetric. `mid_dinv`: each block is symmetric. `leaf_dinv`: each block is symmetric. `top_pattern`: each row holds 3 distinct increasing numbers of 0 to 3. mid_parent[j] is 2 * (j // 16) plus a number below 2: a level-1 supernode hangs under a level-2 supernode of its own group of 16 devices. leaf_parent[i] is one of the 4 level-1 supernodes numbered from 4 * (i // 8): a leaf hangs under a level-1 supernode of its own group of 4 devices. `mid_pattern`: each row starts with 0 (the parent) and goes on with 2 distinct increasing numbers of 1 to 3. `leaf_pattern`: each row starts with 0 (the parent) and goes on with 2 distinct increasing numbers of 1 to 3. The leaf supernodes of device d are its first leaf_live[d] slots; some device has all 2.
All inputs are finite; a program needn't handle non-finite values.
Results may differ from the reference program's by a relative error of at most 0.0003.
Values sent between devices are 32-bit elements; how exact they have to be, the bound alone decides.
A program may use at most 128 MiB of HBM per device.

```python
import jax
import jax.numpy as jnp
from jax import lax

COLS = 256
SLOTS = 3
GROUP2 = 16
NODES2 = 2
GROUP1 = 4
L0_DEV = 2
ROOTB = 4
TOP = 2
MID = 16
LEAFS = 32


def symmetric_blocks(key, number, extent):
    noise_key, scale_key = jax.random.split(key)
    noise = jax.random.normal(noise_key, (number, extent, extent), jnp.float32)
    diagonal = jax.random.uniform(scale_key, (number, extent), jnp.float32, 1.0, 3.0)
    twin = (noise + jnp.swapaxes(noise, 1, 2)) * (0.45 / jnp.sqrt(extent * 1.0))
    return twin + diagonal[:, :, None] * jnp.eye(extent, dtype=jnp.float32)[None]


def draw_root_frame(key, part):
    blocks = symmetric_blocks(jax.random.fold_in(key, 11), 1, ROOTB * COLS)
    return blocks.reshape(ROOTB * COLS, ROOTB * COLS)


def draw_top_dinv(key, part):
    blocks = symmetric_blocks(jax.random.fold_in(key, 12), TOP, COLS)
    return blocks.reshape(TOP * COLS, COLS)


def draw_mid_dinv(key, part):
    return symmetric_blocks(jax.random.fold_in(key, 13), MID, COLS)


def draw_leaf_dinv(key, part):
    return symmetric_blocks(jax.random.fold_in(key, 14), LEAFS, COLS)


def draw_top_pattern(key, part):
    skipped = jax.random.randint(jax.random.fold_in(key, 33), (TOP, 1), 0, SLOTS + 1)
    later = jnp.arange(0, SLOTS, dtype=jnp.int32)[None, :]
    return (later + (later >= skipped).astype(jnp.int32)).astype(jnp.int32)


def draw_mid_parent(key, part):
    offsets = jax.random.randint(jax.random.fold_in(key, 21), (MID,), 0, NODES2)
    return (jnp.arange(MID, dtype=jnp.int32) // GROUP2 * NODES2 + offsets).astype(jnp.int32)


def draw_leaf_parent(key, part):
    holder = jnp.arange(LEAFS, dtype=jnp.int32) // L0_DEV
    offsets = jax.random.randint(jax.random.fold_in(key, 22), (LEAFS,), 0, GROUP1)
    return (holder // GROUP1 * GROUP1 + offsets).astype(jnp.int32)


def pattern_rows(key, number):
    skipped = jax.random.randint(key, (number, 1), 1, SLOTS + 1)
    later = jnp.arange(1, SLOTS, dtype=jnp.int32)[None, :]
    remaining = later + (later >= skipped).astype(jnp.int32)
    return jnp.concatenate([jnp.zeros((number, 1), jnp.int32), remaining], axis=1).astype(jnp.int32)


def draw_mid_pattern(key, part):
    return pattern_rows(jax.random.fold_in(key, 31), MID)


def draw_leaf_pattern(key, part):
    return pattern_rows(jax.random.fold_in(key, 32), LEAFS)


def draw_leaf_live(key, part):
    first_key, second_key, peak_key = jax.random.split(jax.random.fold_in(key, 41), 3)
    lower_count = jnp.minimum(jax.random.randint(first_key, (MID,), 0, L0_DEV), jax.random.randint(second_key, (MID,), 0, L0_DEV)) + 1
    peak_device = jax.random.randint(peak_key, (), 0, MID)
    return jnp.where(jnp.arange(MID, dtype=jnp.int32) == peak_device, L0_DEV, lower_count).astype(jnp.int32)


def with_ends(array, rng, least, high):
    dims = array.shape
    place = [jax.random.randint(jax.random.fold_in(rng, axis), (), 0, dims[axis]) for axis in range(len(dims))]
    array = array.at[tuple(place)].set(least)
    longest = dims.index(max(dims))
    place[longest] = (place[longest] + 1) % dims[longest]
    return array.at[tuple(place)].set(high)


def level_of(rng, shape, cuts, low, top_value):
    loudness = 1.0
    for position, shards_of in cuts:
        draws = jax.random.uniform(jax.random.fold_in(jax.random.fold_in(rng, 6), position), (shards_of,), jnp.float32, low / len(cuts), top_value / len(cuts))
        loudness = loudness * jnp.repeat(jnp.exp(draws), shape[position] // shards_of).reshape((-1,) + (1,) * (len(shape) - 1 - position))
    return loudness


def bell_draw(own_key, shape, scale, bound, shards=(), held_as=jnp.bfloat16):
    drawn = scale * jax.random.normal(own_key, shape, jnp.float32)
    if shards:
        drawn = drawn * level_of(own_key, shape, shards, -0.22, 0.18)
    return jnp.clip(drawn, -bound, bound).astype(held_as)


def setup_inputs(seed: int = 0, part: int = 0) -> dict:
    keys = jax.random.split(jax.random.key(seed), 17)
    part_splits = jax.random.split(jax.random.fold_in(keys[16], part), 17)
    root_frame = draw_root_frame(jax.random.fold_in(jax.random.fold_in(keys[16], part), 71), part)
    top_lhat = bell_draw(part_splits[1], (TOP * SLOTS * COLS, COLS), (SLOTS * COLS) ** -0.5, 0.21875, ((0, 16),), jnp.float32)
    top_dinv = draw_top_dinv(jax.random.fold_in(jax.random.fold_in(keys[16], part), 71), part)
    mid_lhat = bell_draw(part_splits[3], (MID, SLOTS * COLS, COLS), (SLOTS * COLS) ** -0.5, 0.21875, ((0, 16),), jnp.float32)
    mid_dinv = draw_mid_dinv(jax.random.fold_in(jax.random.fold_in(keys[16], part), 71), part)
    leaf_lhat = bell_draw(part_splits[5], (LEAFS, SLOTS * COLS, COLS), (SLOTS * COLS) ** -0.5, 0.21875, ((0, 16),), jnp.float32)
    leaf_dinv = draw_leaf_dinv(jax.random.fold_in(jax.random.fold_in(keys[16], part), 71), part)
    top_columns = jax.random.randint(keys[7], (TOP,), COLS // 2, COLS + 1).astype(jnp.int32)
    mid_columns = with_ends(jax.random.randint(keys[8], (MID,), COLS // 2, COLS + 1), jax.random.fold_in(keys[8], 1), COLS // 2, COLS).astype(jnp.int32)
    leaf_columns = with_ends(jax.random.randint(keys[9], (LEAFS,), COLS // 2, COLS + 1), jax.random.fold_in(keys[9], 1), COLS // 2, COLS).astype(jnp.int32)
    top_pattern = draw_top_pattern(jax.random.fold_in(keys[16], 71), part)
    mid_parent = draw_mid_parent(jax.random.fold_in(keys[16], 71), part)
    leaf_parent = draw_leaf_parent(jax.random.fold_in(keys[16], 71), part)
    mid_pattern = draw_mid_pattern(jax.random.fold_in(keys[16], 71), part)
    leaf_pattern = draw_leaf_pattern(jax.random.fold_in(keys[16], 71), part)
    leaf_live = draw_leaf_live(jax.random.fold_in(keys[16], 71), part)
    return dict(root_frame=root_frame, top_lhat=top_lhat, top_dinv=top_dinv, mid_lhat=mid_lhat, mid_dinv=mid_dinv, leaf_lhat=leaf_lhat, leaf_dinv=leaf_dinv, top_columns=top_columns, mid_columns=mid_columns, leaf_columns=leaf_columns, top_pattern=top_pattern, mid_parent=mid_parent, leaf_parent=leaf_parent, mid_pattern=mid_pattern, leaf_pattern=leaf_pattern, leaf_live=leaf_live)


highest = lax.Precision.HIGHEST


def masked_inputs(lhat_block, dinv_block, used_width):
    block_size = lhat_block.shape[-1]
    column_keep = (jnp.arange(block_size, dtype=jnp.int32) < used_width).astype(lhat_block.dtype)
    lhat_masked = lhat_block * column_keep[None, :]
    dinv_masked = dinv_block * column_keep[:, None] * column_keep[None, :]
    return lhat_masked, dinv_masked


def solve_node(local_frame, lhat_block, dinv_block, used_width):
    lhat_masked, dinv_masked = masked_inputs(lhat_block, dinv_block, used_width)
    coupling = -jnp.dot(local_frame, lhat_masked, precision=highest, preferred_element_type=jnp.float32)
    diagonal = dinv_masked - jnp.dot(lhat_masked.T, coupling, precision=highest, preferred_element_type=jnp.float32)
    return diagonal, coupling


def extended_matrix(diagonal, coupling, local_frame):
    upper_row = jnp.concatenate([diagonal, coupling.T], axis=1)
    lower_row = jnp.concatenate([coupling, local_frame], axis=1)
    return jnp.concatenate([upper_row, lower_row], axis=0)


def select_frame(matrix, pattern, block_size):
    row_ids = (pattern[:, None].astype(jnp.int32) * block_size + jnp.arange(block_size, dtype=jnp.int32)[None, :]).reshape(-1).astype(jnp.int32)
    picked = jnp.take(matrix, row_ids, axis=0)
    return jnp.take(picked, row_ids, axis=1)


def reference(root_frame, top_lhat, top_dinv, mid_lhat, mid_dinv, leaf_lhat, leaf_dinv, top_columns, mid_columns, leaf_columns, top_pattern, mid_parent, leaf_parent, mid_pattern, leaf_pattern, leaf_live):
    frame_size = SLOTS * COLS
    frame_nodes = lax.map(lambda pattern: select_frame(root_frame, pattern, COLS), top_pattern)
    lhat_nodes = top_lhat.reshape(TOP, frame_size, COLS)
    dinv_nodes = top_dinv.reshape(TOP, COLS, COLS)
    top_diag, top_coup = jax.vmap(solve_node)(frame_nodes, lhat_nodes, dinv_nodes, top_columns)
    upper_mats = jax.vmap(extended_matrix)(top_diag, top_coup, frame_nodes)

    def mid_one(node_index):
        parent = mid_parent[node_index]
        local_frame = select_frame(upper_mats[parent], mid_pattern[node_index], COLS)
        return solve_node(local_frame, mid_lhat[node_index], mid_dinv[node_index], mid_columns[node_index])

    mid_diag, mid_coup = lax.map(mid_one, jnp.arange(MID, dtype=jnp.int32))

    def leaf_one(node_index):
        parent = leaf_parent[node_index]
        above_frame = select_frame(upper_mats[mid_parent[parent]], mid_pattern[parent], COLS)
        matrix = extended_matrix(mid_diag[parent], mid_coup[parent], above_frame)
        local_frame = select_frame(matrix, leaf_pattern[node_index], COLS)
        diagonal, coupling = solve_node(local_frame, leaf_lhat[node_index], leaf_dinv[node_index], leaf_columns[node_index])
        live_mask = (node_index % L0_DEV < leaf_live[node_index // L0_DEV]).astype(diagonal.dtype)
        return diagonal * live_mask, coupling * live_mask

    leaf_diag, leaf_coup = lax.map(leaf_one, jnp.arange(LEAFS, dtype=jnp.int32))
    return (top_diag.reshape(TOP * COLS, COLS), top_coup.reshape(TOP * frame_size, COLS), mid_diag, mid_coup, leaf_diag, leaf_coup)
```

```python
import functools

import jax
import jax.numpy as jnp
from jax import lax
from jax.experimental import pallas as pl
from jax.experimental.pallas import tpu as pltpu
from jax.sharding import PartitionSpec as P

SLOTS = 3
GROUP2 = 16
NODES2 = 2
GROUP1 = 4
TILE = 128
OWN = 2 * SLOTS + 1

MESH = pl.DeviceIdType.MESH
f32 = jnp.float32
bf16 = jnp.bfloat16


def split(value):
    high = value.astype(bf16)
    low = (value - high.astype(f32)).astype(bf16)
    return high, low


def in_hbm(x):
    return pltpu.with_memory_space_constraint(x, pltpu.HBM)


def root_windows(tiles):
    if tiles == 8:
        return [(0, 7), (1, 7), (2, 6), (3, 6), (4, 6), (5, 6), (2, 7), (0, 8)]
    return [(r, tiles) for r in range(tiles)]


def half_windows(tiles):
    return [(r, tiles) for r in range(tiles)]


class Part:
    def __init__(self, own, place, group, sems, me, total, rows=0, windows=None):
        self.own, self.place, self.group, self.total = own, place, group, total
        self.recv, self.recv_core, self.line, self.side, self.core, self.local = sems
        self.base = me - lax.rem(me, group)
        self.rows, self.windows = rows, windows
        self.me = me

    def cases(self, device, act):
        if self.windows is None:
            act(None)
            return
        row = lax.rem(lax.div((device - self.base) * self.rows, TILE), len(self.windows))
        for i, window in enumerate(self.windows):
            pl.when(row == i)(functools.partial(act, window))

    def view(self, ref, window):
        if window is None:
            return ref
        return ref.at[:, window[0] * TILE : window[1] * TILE]

    def copy(self, device, window, target, send, recv, own=False):
        dst = self.view(self.place(device - self.base), window)
        return pltpu.make_async_remote_copy(
            src_ref=self.view(self.own, window) if own else dst,
            dst_ref=dst,
            send_sem=send,
            recv_sem=recv,
            device_id={"leaf": target},
            device_id_type=MESH,
        )

    def slot(self, device):
        return lax.div(device - self.base, 2)

    def to_line(self, device, window, target, way, own):
        slot = self.slot(device)
        index = slot
        if isinstance(way, int) and way == 1:
            index = self.group // 2 + lax.rem(slot, 2)
        return self.copy(
            device, window, target, self.line.at[index], self.recv.at[slot], own
        )

    def to_side(self, device, window, target, own):
        index = lax.div(device - self.base, GROUP1) if self.side.shape[0] > 1 else 0
        slot = self.slot(device)
        return self.copy(device, window, target, self.side.at[index], self.recv.at[slot], own)

    def to_core(self, device, window, target, own):
        return self.copy(device, window, target, self.core.at[0], self.recv_core.at[0], own)

    def arrived(self, device, window):
        self.to_line(device, window, self.me, 0, False).wait_recv()

    def all_core(self):
        return pltpu.make_async_remote_copy(
            src_ref=self.total,
            dst_ref=self.total,
            send_sem=self.core.at[0],
            recv_sem=self.recv_core.at[0],
            device_id={"leaf": self.me},
            device_id_type=MESH,
        )

    def keep(self, window):
        return pltpu.make_async_copy(
            self.view(self.own, window),
            self.view(self.place(self.me - self.base), window),
            self.local.at[0],
        )


def start(copy):
    copy.start()


def wait_send(copy):
    copy.wait_send()


def dinv_of(block, cols):
    half = cols // 2
    top = block[:half]
    low = jnp.concatenate([top[:, half:].T, block[half:, half:]], axis=1)
    return jnp.concatenate([top, low], axis=0)


def solve_all(cols, lcats, jobs, after=None):
    row_ids = lax.broadcasted_iota(jnp.int32, (cols, cols), 0)
    lane_ids = lax.broadcasted_iota(jnp.int32, (cols, cols), 1)
    for i, (blocks, lhat, dinv, used, put_coup, put_diag, put) in enumerate(jobs):
        for r in range(SLOTS):
            high, low = split(jnp.where(lane_ids < used, lhat(r), 0.0))
            for part, value in enumerate((high, low, high)):
                first = (3 * r + part) * cols
                lcats[i, first : first + cols] = value
    turned = [[] for _ in jobs]
    for r in range(SLOTS):
        for i, (blocks, lhat, dinv, used, put_coup, put_diag, put) in enumerate(jobs):
            parts = []
            for k in range(SLOTS):
                high, low = blocks(r, k)
                parts += [high, high, low]
            wide = jnp.concatenate(parts, axis=1)
            coup = -jnp.dot(wide, lcats[i], preferred_element_type=f32)
            put_coup(r, coup)
            high, low = split(coup)
            high_t, low_t = high.T, low.T
            if put is not None:
                put(1 + r, high, low)
                put(1 + SLOTS + r, high_t, low_t)
            turned[i] += [high_t, high_t, low_t]
        if after is not None:
            after(r)
    for i, (blocks, lhat, dinv, used, put_coup, put_diag, put) in enumerate(jobs):
        wide = jnp.concatenate(turned[i], axis=1)
        product = jnp.dot(wide, lcats[i], preferred_element_type=f32)
        keep = (lane_ids < used) & (row_ids < used)
        diag = jnp.where(keep, dinv(), 0.0) - product
        put_diag(diag)
        if put is not None:
            put(0, *split(diag))


def gather_kernel(
    n,
    columns_in,
    pattern_in,
    root_in,
    tl_in,
    td_in,
    ml_in,
    md_in,
    pool_h,
    pool_l,
    top_coup_out,
    top_diag_out,
    ml_all,
    md_all,
    root_all,
    tl_all,
    td_all,
    top_c,
    top_d,
    lcats,
    columns,
    pattern,
    small_sems,
    *sems,
):
    me = lax.axis_index("leaf")
    core = lax.rem(me, 2)
    side = lax.rem(lax.div(me, 2), 2)
    cpeer = me + 1 - 2 * core
    xpeer = me + 2 - 4 * side
    other = cpeer + xpeer - me
    cols = td_in.shape[1]
    frame = SLOTS * cols
    half = cols // 2
    per = root_in.shape[1] // cols

    def rows_of(ref, rows):
        return lambda slot: ref.at[pl.ds(pl.multiple_of(slot * rows, 8), rows)]

    def next_sems():
        nonlocal sems
        taken, sems = sems[:6], sems[6:]
        return taken

    def by_rows(own, whole, group, windows=None):
        rows, width = own.shape
        tiles = width // TILE
        widths = [c1 - c0 for c0, c1 in windows] if windows else [tiles]
        half_of = group * rows // 2 * sum(widths) // (len(widths) * tiles)
        place = rows_of(whole, rows)
        return Part(own, place, group, next_sems(), me, whole.at[0:half_of], rows, windows)

    root = by_rows(root_in, root_all, n, root_windows(per * cols // TILE))
    tl = by_rows(tl_in, tl_all, GROUP2)
    td = by_rows(td_in, td_all, GROUP2, half_windows(cols // TILE))

    def mid_part(own, whole, *index):
        place = lambda slot: whole.at[(slot,) + index]
        total = whole.at[(slice(0, 2),) + index]
        return Part(own.at[index], place, GROUP1, next_sems(), me, total)

    cut = 2 * cols
    md0 = mid_part(md_in, md_all, slice(0, half))
    md1 = mid_part(md_in, md_all, slice(half, cols), slice(half, cols))
    ml0 = mid_part(ml_in, ml_all, slice(0, cut))
    ml1 = mid_part(ml_in, ml_all, slice(cut, frame))
    mids = (md0, md1, ml0, ml1)

    line = n // GROUP1
    place = lax.div(me, GROUP1)
    top_line = GROUP2 // GROUP1
    top_place = lax.div(lax.rem(me, GROUP2), GROUP1)
    has_next = (place < line - 1, place > 0)
    top_next = (top_place < top_line - 1, top_place > 0)

    fetches = [
        pltpu.make_async_copy(a, b, small_sems.at[i])
        for i, (a, b) in enumerate([(columns_in, columns), (pattern_in, pattern)])
    ]
    for fetch in fetches:
        fetch.start()

    barrier = pltpu.get_barrier_semaphore()

    def greet(target):
        pl.semaphore_signal(barrier, inc=1, device_id={"leaf": target}, device_id_type=MESH)

    greet(cpeer)
    greet(xpeer)
    pl.when(has_next[0])(lambda: greet(me + GROUP1))
    pl.when(has_next[1])(lambda: greet(me - GROUP1))
    both = (root, tl)
    single = (td,)
    everything = single + both + mids
    for part in everything:
        part.cases(me, lambda w, part=part: part.keep(w).start())
    peers = 2 + jnp.minimum(place, 1) + jnp.minimum(line - 1 - place, 1)
    pl.semaphore_wait(barrier, peers)

    def along(part, device, window, way, act, own=False):
        up, down = has_next if part.group == n else top_next
        if isinstance(way, int):
            ok, target = (down, me - GROUP1) if way else (up, me + GROUP1)
        else:
            ok, target = jnp.where(way == 0, up, down), me + GROUP1 - 2 * GROUP1 * way
        pl.when(ok)(lambda: act(part.to_line(device, window, target, way, own)))

    def side_to(part, device, window, act, own=False):
        act(part.to_side(device, window, xpeer, own))

    def core_to(part, device, window, act, own=False):
        if act is start:
            act(part.to_core(device, window, cpeer, own))

    def own_moves(part, act, lines=True, side=True, core=True):
        def moves(window):
            if lines:
                along(part, me, window, 0, act, True)
                along(part, me, window, 1, act, True)
            if side:
                side_to(part, me, window, act, True)
            if core:
                core_to(part, me, window, act, True)

        part.cases(me, moves)

    for part in both:
        own_moves(part, start, lines=False, core=False)
    for part in single + both:
        own_moves(part, start, side=False, core=False)
    for part in single + mids:
        own_moves(part, start, lines=False, core=False)
    for part in everything:
        own_moves(part, start, lines=False, side=False)

    def passed(part, device, way, act, side=False, wait=False):
        def moves(window):
            if wait:
                part.arrived(device, window)
            if way is None:
                along(part, device, window, 0, act)
                along(part, device, window, 1, act)
            else:
                along(part, device, window, way, act)
            if side:
                side_to(part, device, window, act)
            core_to(part, device, window, act)

        part.cases(device, moves)

    for part in both:
        passed(part, xpeer, None, start, wait=True)

    outer = lax.div(2 * place, line)

    def steps(act, wait):
        def step(s, carry):
            def turn(t, carry):
                way = lax.rem(t + 1 + outer, 2)
                shift = (2 * way - 1) * s * GROUP1
                got_top = jnp.where(way == 0, top_place >= s, top_place + s < top_line)
                got_root = jnp.where(way == 0, place >= s, place + s < line)

                @pl.when(got_top)
                def _():
                    for part in single:
                        passed(part, me + shift, way, act, side=True, wait=wait)

                def one(i, carry):
                    device = jnp.where(i == 0, me, xpeer) + shift

                    @pl.when(got_root)
                    def _():
                        passed(root, device, way, act, wait=wait)

                    @pl.when(got_top)
                    def _():
                        passed(tl, device, way, act, wait=wait)

                    return carry

                lax.fori_loop(0, 2, one, 0)
                return carry

            lax.fori_loop(0, 2, turn, 0)
            return carry

        lax.fori_loop(1, line, step, 0)

    steps(start, True)

    def crossed(part, device, act, wait):
        def moves(window):
            if wait:
                part.arrived(device, window)
            core_to(part, device, window, act)

        part.cases(device, moves)

    def tops_crossed(act, wait):
        for q in range(top_line):
            for part in single:
                crossed(part, part.base + q * GROUP1 + lax.rem(xpeer, GROUP1), act, wait)

    tops_crossed(start, True)
    for part in mids[:3]:
        crossed(part, xpeer, start, True)

    def from_core(part):
        part.all_core().wait_recv()
        part.cases(me, lambda w: part.keep(w).wait())

    from_core(root)
    tiles = cols // TILE
    windows = root.windows
    for r, (c0, c1) in enumerate(windows):
        for c in range(c0, c1):
            value = root_all[r * TILE : (r + 1) * TILE, c * TILE : (c + 1) * TILE]
            for a, b, tile in ((r, c, value), (c, r, value.T))[: 1 if r == c else 2]:
                high, low = split(tile)
                index = (a // tiles) * per + b // tiles
                rows = slice(a % tiles * TILE, (a % tiles + 1) * TILE)
                lanes = slice(b % tiles * TILE, (b % tiles + 1) * TILE)
                pool_h[index, rows, lanes] = high
                pool_l[index, rows, lanes] = low
    for fetch in fetches:
        fetch.wait()
    for part in single + (tl,):
        from_core(part)

    top_base = lax.div(me, GROUP2) * NODES2
    roots = per * per

    def top_job(q):
        chosen = [pattern[top_base + q, k] for k in range(SLOTS)]

        def blocks(r, k):
            index = chosen[r] * per + chosen[k]
            return pool_h[index], pool_l[index]

        def lhat(r):
            return tl_all[q * frame + r * cols : q * frame + (r + 1) * cols]

        def put_coup(r, value):
            top_c[q * frame + r * cols : q * frame + (r + 1) * cols] = value

        def put_diag(value):
            top_d[q * cols : (q + 1) * cols] = value

        def put(which, high, low):
            pool_h[roots + q * OWN + which] = high
            pool_l[roots + q * OWN + which] = low

        def dinv():
            return dinv_of(td_all[q * cols : (q + 1) * cols], cols)

        return blocks, lhat, dinv, columns[top_base + q], put_coup, put_diag, put

    solve_all(cols, lcats, [top_job(q) for q in range(NODES2)])
    member = lax.rem(me, GROUP2)
    rows = top_coup_out.shape[0]
    top_coup_out[...] = top_c[pl.ds(pl.multiple_of(member * rows, 8), rows)]
    rows = top_diag_out.shape[0]
    top_diag_out[...] = top_d[pl.ds(pl.multiple_of(member * rows, 8), rows)]

    crossed(ml1, xpeer, start, True)
    for part in mids:
        from_core(part)

    for part in both:
        own_moves(part, wait_send)
        passed(part, xpeer, None, wait_send)
    for part in single:
        own_moves(part, wait_send)
    for part in mids:
        own_moves(part, wait_send, lines=False)
    steps(wait_send, False)
    for part in everything:
        part.all_core().wait_send()


def tree_kernel(per, *refs):
    small_in, refs = refs[:8], refs[8:]
    pool_h, pool_l, top_coup, top_diag, ml_all, md_all, leaf_lhat_in, leaf_dinv_in = refs[:8]
    top_diag_out, top_coup_out, mid_diag_out, mid_coup_out, leaf_diag_out, leaf_coup_out = refs[8:14]
    e1h, e1l, lcats, leaf_lhat, leaf_dinv, mid_c, mid_d, leaf_c, leaf_d = refs[14:23]
    small = refs[23:31]
    in_sems, out_sems = refs[31:]
    (
        mid_columns,
        leaf_columns,
        top_pattern,
        mid_parent,
        leaf_parent,
        mid_pattern,
        leaf_pattern,
        leaf_live,
    ) = small
    fetched = list(zip(small_in + (leaf_lhat_in, leaf_dinv_in), small + (leaf_lhat, leaf_dinv)))
    fetches = [pltpu.make_async_copy(a, b, in_sems.at[i]) for i, (a, b) in enumerate(fetched)]
    for fetch in fetches:
        fetch.start()
    tops = [
        pltpu.make_async_copy(top_coup, top_coup_out, out_sems.at[0]),
        pltpu.make_async_copy(top_diag, top_diag_out, out_sems.at[1]),
    ]
    for copy in tops:
        copy.start()
    me = lax.axis_index("leaf")
    leaves, cols = leaf_dinv.shape[0], leaf_dinv.shape[2]
    roots = per * per
    top_base = lax.div(me, GROUP2) * NODES2
    mid_base = lax.div(me, GROUP1) * GROUP1
    mine = lax.rem(me, GROUP1)
    for fetch in fetches[:-2]:
        fetch.wait()
    live = leaf_live[me]

    def pool_index(node, u, v):
        parent = mid_parent[node] - top_base
        a = mid_pattern[u, node]
        b = mid_pattern[v, node]
        base = roots + parent * OWN
        near = base + jnp.where(b == 0, a, SLOTS + b)
        far_a = top_pattern[top_base + parent, jnp.maximum(a - 1, 0)]
        far_b = top_pattern[top_base + parent, jnp.maximum(b - 1, 0)]
        return jnp.where((a == 0) | (b == 0), near, far_a * per + far_b)

    parents = [leaf_parent[me * leaves + i] - mid_base for i in range(leaves)]

    def mid_job(k):
        local = parents[k - 1] if k else mine
        node = mid_base + local

        def blocks(r, c):
            index = pool_index(node, r, c)
            return pool_h[index], pool_l[index]

        def lhat(r):
            return ml_all[local, r * cols : (r + 1) * cols]

        def put_coup(r, value):
            if k == 0:
                mid_c[r * cols : (r + 1) * cols] = value

        def put_diag(value):
            if k == 0:
                mid_d[...] = value

        def put(which, high, low):
            e1h[k, which] = high
            e1l[k, which] = low

        def dinv():
            return dinv_of(md_all[local], cols)

        return blocks, lhat, dinv, mid_columns[node], put_coup, put_diag, put

    solve_all(cols, lcats, [mid_job(k) for k in range(leaves + 1)])
    outs = [
        pltpu.make_async_copy(mid_c, mid_coup_out, out_sems.at[2]),
        pltpu.make_async_copy(mid_d, mid_diag_out, out_sems.at[3]),
    ]
    for copy in outs:
        copy.start()
    for fetch in fetches[-2:]:
        fetch.wait()

    def leaf_job(i):
        node = me * leaves + i
        above = mid_base + parents[i]
        alive = jnp.full((cols, cols), i, jnp.int32) < live

        def blocks(r, c):
            if r == 0 or c == 0:
                if r == 0:
                    which = leaf_pattern[c, node] + SLOTS if c else 0
                else:
                    which = leaf_pattern[r, node]
                return e1h[i + 1, which], e1l[i + 1, which]
            index = pool_index(above, leaf_pattern[r, node] - 1, leaf_pattern[c, node] - 1)
            return pool_h[index], pool_l[index]

        def lhat(r):
            return leaf_lhat[i, r * cols : (r + 1) * cols]

        def put_coup(r, value):
            leaf_c[i, r * cols : (r + 1) * cols] = jnp.where(alive, value, 0.0)

        def put_diag(value):
            leaf_d[i] = jnp.where(alive, value, 0.0)

        def dinv():
            return leaf_dinv[i]

        return blocks, lhat, dinv, leaf_columns[node], put_coup, put_diag, None

    def leaf_rows(r):
        for i in range(leaves):
            rows = pl.ds(r * cols, cols)
            copy = pltpu.make_async_copy(
                leaf_c.at[i, rows],
                leaf_coup_out.at[i, rows],
                out_sems.at[4 + i * (SLOTS + 1) + r],
            )
            copy.start()
            outs.append(copy)

    def after(r):
        if r:
            leaf_rows(r - 1)

    solve_all(cols, lcats, [leaf_job(i) for i in range(leaves)], after)
    leaf_rows(SLOTS - 1)
    for i in range(leaves):
        copy = pltpu.make_async_copy(
            leaf_d.at[i], leaf_diag_out.at[i], out_sems.at[4 + i * (SLOTS + 1) + SLOTS]
        )
        copy.start()
        outs.append(copy)
    for copy in tops + outs:
        copy.wait()


def body(
    root_frame,
    top_lhat,
    top_dinv,
    mid_lhat,
    mid_dinv,
    leaf_lhat,
    leaf_dinv,
    top_columns,
    mid_columns,
    leaf_columns,
    top_pattern,
    mid_parent,
    leaf_parent,
    mid_pattern,
    leaf_pattern,
    leaf_live,
):
    n = lax.axis_size("leaf")
    cols = top_dinv.shape[1]
    frame = SLOTS * cols
    per = root_frame.shape[1] // cols
    leaves = leaf_lhat.shape[0]
    pool = per * per + NODES2 * OWN

    def dma(count):
        return pltpu.SemaphoreType.DMA((count,))

    def part_sems(group, line, side):
        return [dma(group // 2), dma(1), dma(line), dma(side), dma(1), dma(1)]

    sems = part_sems(n, n // 2 + 2, 1) + part_sems(GROUP2, GROUP2 // 2 + 2, 1)
    sems += part_sems(GROUP2, GROUP2 // 2 + 2, GROUP2 // GROUP1)
    for _ in range(4):
        sems += part_sems(GROUP1, 1, 1)
    vmem = pl.BlockSpec(memory_space=pltpu.VMEM)
    hbm = pl.BlockSpec(memory_space=pltpu.HBM)
    shape = jax.ShapeDtypeStruct
    moved = (top_columns, top_pattern, root_frame, top_lhat, top_dinv, mid_lhat[0], mid_dinv[0])
    pool_h, pool_l, top_coup, top_diag, ml_all, md_all = pl.pallas_call(
        functools.partial(gather_kernel, n),
        out_shape=[
            shape((pool, cols, cols), bf16),
            shape((pool, cols, cols), bf16),
            shape(top_lhat.shape, f32),
            shape(top_dinv.shape, f32),
            shape((GROUP1, frame, cols), f32),
            shape((GROUP1, cols, cols), f32),
        ],
        in_specs=[hbm] * 7,
        out_specs=[vmem] * 6,
        scratch_shapes=[
            pltpu.VMEM((per * cols, per * cols), f32),
            pltpu.VMEM((NODES2 * frame, cols), f32),
            pltpu.VMEM((NODES2 * cols, cols), f32),
            pltpu.VMEM((NODES2 * frame, cols), f32),
            pltpu.VMEM((NODES2 * cols, cols), f32),
            pltpu.VMEM((NODES2, 3 * frame, cols), bf16),
            pltpu.SMEM(top_columns.shape, jnp.int32),
            pltpu.SMEM(top_pattern.shape, jnp.int32),
            dma(2),
        ]
        + sems,
        compiler_params=pltpu.CompilerParams(
            collective_id=0, has_side_effects=True, vmem_limit_bytes=20 * 1024 * 1024
        ),
    )(*[in_hbm(x) for x in moved])
    small = (
        mid_columns,
        leaf_columns,
        top_pattern,
        mid_parent,
        leaf_parent,
        mid_pattern.T,
        leaf_pattern.T,
        leaf_live,
    )
    outs = pl.pallas_call(
        functools.partial(tree_kernel, per),
        out_shape=[
            shape(top_dinv.shape, f32),
            shape(top_lhat.shape, f32),
            shape(mid_dinv.shape[1:], f32),
            shape(mid_lhat.shape[1:], f32),
            shape(leaf_dinv.shape, f32),
            shape(leaf_lhat.shape, f32),
        ],
        in_specs=[hbm] * 8 + [vmem] * 6 + [hbm] * 2,
        out_specs=[hbm] * 6,
        scratch_shapes=[
            pltpu.VMEM((leaves + 1, OWN, cols, cols), bf16),
            pltpu.VMEM((leaves + 1, OWN, cols, cols), bf16),
            pltpu.VMEM((leaves + 1, 3 * frame, cols), bf16),
            pltpu.VMEM(leaf_lhat.shape, f32),
            pltpu.VMEM(leaf_dinv.shape, f32),
            pltpu.VMEM((frame, cols), f32),
            pltpu.VMEM((cols, cols), f32),
            pltpu.VMEM(leaf_lhat.shape, f32),
            pltpu.VMEM(leaf_dinv.shape, f32),
        ]
        + [pltpu.SMEM(x.shape, jnp.int32) for x in small]
        + [dma(len(small) + 2), dma(4 + leaves * (SLOTS + 1))],
        compiler_params=pltpu.CompilerParams(vmem_limit_bytes=24 * 1024 * 1024),
    )(
        *[in_hbm(x) for x in small],
        pool_h,
        pool_l,
        top_coup,
        top_diag,
        ml_all,
        md_all,
        in_hbm(leaf_lhat),
        in_hbm(leaf_dinv),
    )
    return (outs[0], outs[1], outs[2][None], outs[3][None], outs[4], outs[5])


def solution(mesh):
    rows = P(("pole", "leaf"), None)
    stacks = P(("pole", "leaf"), None, None)
    in_specs = (rows,) * 3 + (stacks,) * 4 + (P(),) * 9
    out_specs = (rows,) * 2 + (stacks,) * 4
    return jax.shard_map(body, mesh=mesh, in_specs=in_specs, out_specs=out_specs, check_vma=False)
```

```python
import functools

import jax
import jax.numpy as jnp
from jax import lax
from jax.experimental import pallas as pl
from jax.experimental.pallas import tpu as pltpu
from jax.sharding import PartitionSpec as P

SLOTS = 3
GROUP2 = 16
NODES2 = 2
GROUP1 = 4
TILE = 128
OWN = 2 * SLOTS + 1

MESH = pl.DeviceIdType.MESH
f32 = jnp.float32
bf16 = jnp.bfloat16


def split(value):
    high = value.astype(bf16)
    low = (value - high.astype(f32)).astype(bf16)
    return high, low


def in_hbm(x):
    return pltpu.with_memory_space_constraint(x, pltpu.HBM)


def root_windows(tiles):
    if tiles == 8:
        return [(0, 7), (1, 7), (2, 6), (3, 6), (4, 6), (5, 6), (2, 7), (0, 8)]
    return [(r, tiles) for r in range(tiles)]


def half_windows(tiles):
    return [(r, tiles) for r in range(tiles)]


class Part:
    def __init__(self, own, place, group, sems, me, total, rows=0, windows=None):
        self.own, self.place, self.group, self.total = own, place, group, total
        self.recv, self.recv_core, self.line, self.side, self.core, self.local = sems
        self.base = me - lax.rem(me, group)
        self.rows, self.windows = rows, windows
        self.me = me

    def cases(self, device, act):
        if self.windows is None:
            act(None)
            return
        row = lax.rem(lax.div((device - self.base) * self.rows, TILE), len(self.windows))
        for i, window in enumerate(self.windows):
            pl.when(row == i)(functools.partial(act, window))

    def view(self, ref, window):
        if window is None:
            return ref
        return ref.at[:, window[0] * TILE : window[1] * TILE]

    def copy(self, device, window, target, send, recv, own=False):
        dst = self.view(self.place(device - self.base), window)
        return pltpu.make_async_remote_copy(
            src_ref=self.view(self.own, window) if own else dst,
            dst_ref=dst,
            send_sem=send,
            recv_sem=recv,
            device_id={"leaf": target},
            device_id_type=MESH,
        )

    def slot(self, device):
        return lax.div(device - self.base, 2)

    def to_line(self, device, window, target, way, own):
        slot = self.slot(device)
        index = slot
        if isinstance(way, int) and way == 1:
            index = self.group // 2 + lax.rem(slot, 2)
        return self.copy(
            device, window, target, self.line.at[index], self.recv.at[slot], own
        )

    def to_side(self, device, window, target, own):
        index = lax.div(device - self.base, GROUP1) if self.side.shape[0] > 1 else 0
        slot = self.slot(device)
        return self.copy(device, window, target, self.side.at[index], self.recv.at[slot], own)

    def to_core(self, device, window, target, own):
        return self.copy(device, window, target, self.core.at[0], self.recv_core.at[0], own)

    def arrived(self, device, window):
        self.to_line(device, window, self.me, 0, False).wait_recv()

    def all_core(self):
        return pltpu.make_async_remote_copy(
            src_ref=self.total,
            dst_ref=self.total,
            send_sem=self.core.at[0],
            recv_sem=self.recv_core.at[0],
            device_id={"leaf": self.me},
            device_id_type=MESH,
        )

    def keep(self, window):
        return pltpu.make_async_copy(
            self.view(self.own, window),
            self.view(self.place(self.me - self.base), window),
            self.local.at[0],
        )


def start(copy):
    copy.start()


def wait_send(copy):
    copy.wait_send()


def dinv_of(block, cols):
    half = cols // 2
    top = block[:half]
    low = jnp.concatenate([top[:, half:].T, block[half:, half:]], axis=1)
    return jnp.concatenate([top, low], axis=0)


def solve_all(cols, lcats, jobs, after=None):
    row_ids = lax.broadcasted_iota(jnp.int32, (cols, cols), 0)
    lane_ids = lax.broadcasted_iota(jnp.int32, (cols, cols), 1)
    for i, (blocks, lhat, dinv, used, put_coup, put_diag, put) in enumerate(jobs):
        for r in range(SLOTS):
            high, low = split(jnp.where(lane_ids < used, lhat(r), 0.0))
            for part, value in enumerate((high, low, high)):
                first = (3 * r + part) * cols
                lcats[i, first : first + cols] = value
    turned = [[] for _ in jobs]
    for r in range(SLOTS):
        for i, (blocks, lhat, dinv, used, put_coup, put_diag, put) in enumerate(jobs):
            parts = []
            for k in range(SLOTS):
                high, low = blocks(r, k)
                parts += [high, high, low]
            wide = jnp.concatenate(parts, axis=1)
            coup = -jnp.dot(wide, lcats[i], preferred_element_type=f32)
            put_coup(r, coup)
            high, low = split(coup)
            high_t, low_t = high.T, low.T
            if put is not None:
                put(1 + r, high, low)
                put(1 + SLOTS + r, high_t, low_t)
            turned[i] += [high_t, high_t, low_t]
        if after is not None:
            after(r)
    for i, (blocks, lhat, dinv, used, put_coup, put_diag, put) in enumerate(jobs):
        wide = jnp.concatenate(turned[i], axis=1)
        product = jnp.dot(wide, lcats[i], preferred_element_type=f32)
        keep = (lane_ids < used) & (row_ids < used)
        diag = jnp.where(keep, dinv(), 0.0) - product
        put_diag(diag)
        if put is not None:
            put(0, *split(diag))


def gather_kernel(
    n,
    columns_in,
    pattern_in,
    root_in,
    tl_in,
    td_in,
    ml_in,
    md_in,
    pool_h,
    pool_l,
    top_coup_out,
    top_diag_out,
    ml_all,
    md_all,
    root_all,
    tl_all,
    td_all,
    top_c,
    top_d,
    lcats,
    columns,
    pattern,
    small_sems,
    *sems,
):
    me = lax.axis_index("leaf")
    core = lax.rem(me, 2)
    side = lax.rem(lax.div(me, 2), 2)
    cpeer = me + 1 - 2 * core
    xpeer = me + 2 - 4 * side
    other = cpeer + xpeer - me
    cols = td_in.shape[1]
    frame = SLOTS * cols
    half = cols // 2
    per = root_in.shape[1] // cols

    def rows_of(ref, rows, first, count):
        return lambda slot: ref.at[pl.ds(pl.multiple_of(slot * rows + first, 8), count)]

    def next_sems():
        nonlocal sems
        taken, sems = sems[:6], sems[6:]
        return taken

    def by_rows(own, whole, group, windows=None, first=0, last=None):
        rows, width = own.shape
        count = (rows if last is None else last) - first
        tiles = width // TILE
        widths = [c1 - c0 for c0, c1 in windows] if windows else [tiles]
        half_of = group * count // 2 * sum(widths) // (len(widths) * tiles)
        place = rows_of(whole, rows, first, count)
        own = own.at[pl.ds(first, count)]
        return Part(own, place, group, next_sems(), me, whole.at[0:half_of], rows, windows)

    root = by_rows(root_in, root_all, n, root_windows(per * cols // TILE))
    middle = tl_in.shape[0] // 2 // 8 * 8
    tl = by_rows(tl_in, tl_all, GROUP2, None, 0, middle)
    tl_side = by_rows(tl_in, tl_all, GROUP2, None, middle)
    td = by_rows(td_in, td_all, GROUP2, half_windows(cols // TILE))

    def mid_part(own, whole, *index):
        place = lambda slot: whole.at[(slot,) + index]
        total = whole.at[(slice(0, 2),) + index]
        return Part(own.at[index], place, GROUP1, next_sems(), me, total)

    md0 = mid_part(md_in, md_all, slice(0, half))
    md1 = mid_part(md_in, md_all, slice(half, cols), slice(half, cols))
    mls = [mid_part(ml_in, ml_all, slice(r * cols, (r + 1) * cols)) for r in range(SLOTS)]
    mids = (md0, md1) + tuple(mls)

    line = n // GROUP1
    place = lax.div(me, GROUP1)
    top_line = GROUP2 // GROUP1
    top_place = lax.div(lax.rem(me, GROUP2), GROUP1)
    has_next = (place < line - 1, place > 0)
    top_next = (top_place < top_line - 1, top_place > 0)

    fetches = [
        pltpu.make_async_copy(a, b, small_sems.at[i])
        for i, (a, b) in enumerate([(columns_in, columns), (pattern_in, pattern)])
    ]
    for fetch in fetches:
        fetch.start()

    barrier = pltpu.get_barrier_semaphore()

    def greet(target):
        pl.semaphore_signal(barrier, inc=1, device_id={"leaf": target}, device_id_type=MESH)

    greet(cpeer)
    greet(xpeer)
    pl.when(has_next[0])(lambda: greet(me + GROUP1))
    pl.when(has_next[1])(lambda: greet(me - GROUP1))
    both = (root, tl)
    single = (td, tl_side)
    everything = single + both + mids
    for part in everything:
        part.cases(me, lambda w, part=part: part.keep(w).start())
    peers = 2 + jnp.minimum(place, 1) + jnp.minimum(line - 1 - place, 1)
    pl.semaphore_wait(barrier, peers)

    def along(part, device, window, way, act, own=False):
        up, down = has_next if part.group == n else top_next
        if isinstance(way, int):
            ok, target = (down, me - GROUP1) if way else (up, me + GROUP1)
        else:
            ok, target = jnp.where(way == 0, up, down), me + GROUP1 - 2 * GROUP1 * way
        pl.when(ok)(lambda: act(part.to_line(device, window, target, way, own)))

    def side_to(part, device, window, act, own=False):
        act(part.to_side(device, window, xpeer, own))

    def core_to(part, device, window, act, own=False):
        if act is start:
            act(part.to_core(device, window, cpeer, own))

    def own_moves(part, act, lines=True, side=True, core=True):
        def moves(window):
            if lines:
                along(part, me, window, 0, act, True)
                along(part, me, window, 1, act, True)
            if side:
                side_to(part, me, window, act, True)
            if core:
                core_to(part, me, window, act, True)

        part.cases(me, moves)

    for part in both:
        own_moves(part, start, lines=False, core=False)
    for part in single + both:
        own_moves(part, start, side=False, core=False)
    for part in single + mids[:3]:
        own_moves(part, start, lines=False, core=False)
    for part in everything:
        own_moves(part, start, lines=False, side=False)

    def passed(part, device, way, act, side=False, wait=False):
        def moves(window):
            if wait:
                part.arrived(device, window)
            if way is None:
                along(part, device, window, 0, act)
                along(part, device, window, 1, act)
            else:
                along(part, device, window, way, act)
            if side:
                side_to(part, device, window, act)
            core_to(part, device, window, act)

        part.cases(device, moves)

    for part in both:
        passed(part, xpeer, None, start, wait=True)

    outer = lax.div(2 * place, line)

    last_step = jnp.maximum(top_place, top_line - 1 - top_place)

    def steps(act, wait):
        def step(s, carry):
            def turned(t):
                way = lax.rem(t + 1 + outer, 2)
                shift = (2 * way - 1) * s * GROUP1
                got_top = jnp.where(way == 0, top_place >= s, top_place + s < top_line)
                got_root = jnp.where(way == 0, place >= s, place + s < line)
                return way, shift, got_top, got_root

            def crossing(t, carry):
                way, shift, got_top, _ = turned(t)

                @pl.when(got_top)
                def _():
                    for part in single:
                        passed(part, me + shift, way, act, side=True, wait=wait)

                return carry

            lax.fori_loop(0, 2, crossing, 0)
            if wait:
                @pl.when(s == last_step)
                def _():
                    own_moves(mls[2], start, lines=False, core=False)

            def turn(t, carry):
                way, shift, got_top, got_root = turned(t)

                def one(i, carry):
                    device = jnp.where(i == 0, me, xpeer) + shift

                    @pl.when(got_root)
                    def _():
                        passed(root, device, way, act, wait=wait)

                    @pl.when(got_top)
                    def _():
                        passed(tl, device, way, act, wait=wait)

                    return carry

                lax.fori_loop(0, 2, one, 0)
                return carry

            lax.fori_loop(0, 2, turn, 0)
            if wait:
                @pl.when(s == 1)
                def _():
                    own_moves(mls[1], start, lines=False, core=False)

            return carry

        lax.fori_loop(1, line, step, 0)

    steps(start, True)

    def crossed(part, device, act, wait):
        def moves(window):
            if wait:
                part.arrived(device, window)
            core_to(part, device, window, act)

        part.cases(device, moves)

    def tops_crossed(act, wait):
        for q in range(top_line):
            for part in single:
                crossed(part, part.base + q * GROUP1 + lax.rem(xpeer, GROUP1), act, wait)

    tops_crossed(start, True)
    for part in mids[:4]:
        crossed(part, xpeer, start, True)

    def from_core(part):
        part.all_core().wait_recv()
        part.cases(me, lambda w: part.keep(w).wait())

    from_core(root)
    tiles = cols // TILE
    windows = root.windows
    for r, (c0, c1) in enumerate(windows):
        for c in range(c0, c1):
            value = root_all[r * TILE : (r + 1) * TILE, c * TILE : (c + 1) * TILE]
            for a, b, tile in ((r, c, value), (c, r, value.T))[: 1 if r == c else 2]:
                high, low = split(tile)
                index = (a // tiles) * per + b // tiles
                rows = slice(a % tiles * TILE, (a % tiles + 1) * TILE)
                lanes = slice(b % tiles * TILE, (b % tiles + 1) * TILE)
                pool_h[index, rows, lanes] = high
                pool_l[index, rows, lanes] = low
    for fetch in fetches:
        fetch.wait()
    for part in single + (tl,):
        from_core(part)

    top_base = lax.div(me, GROUP2) * NODES2
    roots = per * per

    def top_job(q):
        chosen = [pattern[top_base + q, k] for k in range(SLOTS)]

        def blocks(r, k):
            index = chosen[r] * per + chosen[k]
            return pool_h[index], pool_l[index]

        def lhat(r):
            return tl_all[q * frame + r * cols : q * frame + (r + 1) * cols]

        def put_coup(r, value):
            top_c[q * frame + r * cols : q * frame + (r + 1) * cols] = value

        def put_diag(value):
            top_d[q * cols : (q + 1) * cols] = value

        def put(which, high, low):
            pool_h[roots + q * OWN + which] = high
            pool_l[roots + q * OWN + which] = low

        def dinv():
            return dinv_of(td_all[q * cols : (q + 1) * cols], cols)

        return blocks, lhat, dinv, columns[top_base + q], put_coup, put_diag, put

    solve_all(cols, lcats, [top_job(q) for q in range(NODES2)])
    member = lax.rem(me, GROUP2)
    rows = top_coup_out.shape[0]
    top_coup_out[...] = top_c[pl.ds(pl.multiple_of(member * rows, 8), rows)]
    rows = top_diag_out.shape[0]
    top_diag_out[...] = top_d[pl.ds(pl.multiple_of(member * rows, 8), rows)]

    crossed(mls[2], xpeer, start, True)
    for part in both:
        own_moves(part, wait_send)
        passed(part, xpeer, None, wait_send)
    for part in single:
        own_moves(part, wait_send)
    for part in mids:
        own_moves(part, wait_send, lines=False)
    steps(wait_send, False)
    for part in mids:
        from_core(part)
    for part in everything:
        part.all_core().wait_send()


def tree_kernel(per, *refs):
    small_in, refs = refs[:8], refs[8:]
    pool_h, pool_l, top_coup, top_diag, ml_all, md_all, leaf_lhat_in, leaf_dinv_in = refs[:8]
    top_diag_out, top_coup_out, mid_diag_out, mid_coup_out, leaf_diag_out, leaf_coup_out = refs[8:14]
    e1h, e1l, lcats, leaf_lhat, leaf_dinv, mid_c, mid_d, leaf_c, leaf_d = refs[14:23]
    small = refs[23:31]
    in_sems, out_sems = refs[31:]
    (
        mid_columns,
        leaf_columns,
        top_pattern,
        mid_parent,
        leaf_parent,
        mid_pattern,
        leaf_pattern,
        leaf_live,
    ) = small
    fetched = list(zip(small_in + (leaf_lhat_in, leaf_dinv_in), small + (leaf_lhat, leaf_dinv)))
    fetches = [pltpu.make_async_copy(a, b, in_sems.at[i]) for i, (a, b) in enumerate(fetched)]
    for fetch in fetches:
        fetch.start()
    tops = [
        pltpu.make_async_copy(top_coup, top_coup_out, out_sems.at[0]),
        pltpu.make_async_copy(top_diag, top_diag_out, out_sems.at[1]),
    ]
    for copy in tops:
        copy.start()
    me = lax.axis_index("leaf")
    leaves, cols = leaf_dinv.shape[0], leaf_dinv.shape[2]
    roots = per * per
    top_base = lax.div(me, GROUP2) * NODES2
    mid_base = lax.div(me, GROUP1) * GROUP1
    mine = lax.rem(me, GROUP1)
    for fetch in fetches[:-2]:
        fetch.wait()
    live = leaf_live[me]

    def pool_index(node, u, v):
        parent = mid_parent[node] - top_base
        a = mid_pattern[u, node]
        b = mid_pattern[v, node]
        base = roots + parent * OWN
        near = base + jnp.where(b == 0, a, SLOTS + b)
        far_a = top_pattern[top_base + parent, jnp.maximum(a - 1, 0)]
        far_b = top_pattern[top_base + parent, jnp.maximum(b - 1, 0)]
        return jnp.where((a == 0) | (b == 0), near, far_a * per + far_b)

    parents = [leaf_parent[me * leaves + i] - mid_base for i in range(leaves)]

    def mid_job(k):
        local = parents[k - 1] if k else mine
        node = mid_base + local

        def blocks(r, c):
            index = pool_index(node, r, c)
            return pool_h[index], pool_l[index]

        def lhat(r):
            return ml_all[local, r * cols : (r + 1) * cols]

        def put_coup(r, value):
            if k == 0:
                mid_c[r * cols : (r + 1) * cols] = value

        def put_diag(value):
            if k == 0:
                mid_d[...] = value

        def put(which, high, low):
            e1h[k, which] = high
            e1l[k, which] = low

        def dinv():
            return dinv_of(md_all[local], cols)

        return blocks, lhat, dinv, mid_columns[node], put_coup, put_diag, put

    solve_all(cols, lcats, [mid_job(k) for k in range(leaves + 1)])
    outs = [
        pltpu.make_async_copy(mid_c, mid_coup_out, out_sems.at[2]),
        pltpu.make_async_copy(mid_d, mid_diag_out, out_sems.at[3]),
    ]
    for copy in outs:
        copy.start()
    for fetch in fetches[-2:]:
        fetch.wait()

    def leaf_job(i):
        node = me * leaves + i
        above = mid_base + parents[i]
        alive = jnp.full((cols, cols), i, jnp.int32) < live

        def blocks(r, c):
            if r == 0 or c == 0:
                if r == 0:
                    which = leaf_pattern[c, node] + SLOTS if c else 0
                else:
                    which = leaf_pattern[r, node]
                return e1h[i + 1, which], e1l[i + 1, which]
            index = pool_index(above, leaf_pattern[r, node] - 1, leaf_pattern[c, node] - 1)
            return pool_h[index], pool_l[index]

        def lhat(r):
            return leaf_lhat[i, r * cols : (r + 1) * cols]

        def put_coup(r, value):
            leaf_c[i, r * cols : (r + 1) * cols] = jnp.where(alive, value, 0.0)

        def put_diag(value):
            leaf_d[i] = jnp.where(alive, value, 0.0)

        def dinv():
            return leaf_dinv[i]

        return blocks, lhat, dinv, leaf_columns[node], put_coup, put_diag, None

    def leaf_rows(r):
        for i in range(leaves):
            rows = pl.ds(r * cols, cols)
            copy = pltpu.make_async_copy(
                leaf_c.at[i, rows],
                leaf_coup_out.at[i, rows],
                out_sems.at[4 + i * (SLOTS + 1) + r],
            )
            copy.start()
            outs.append(copy)

    def after(r):
        if r:
            leaf_rows(r - 1)

    solve_all(cols, lcats, [leaf_job(i) for i in range(leaves)], after)
    leaf_rows(SLOTS - 1)
    for i in range(leaves):
        copy = pltpu.make_async_copy(
            leaf_d.at[i], leaf_diag_out.at[i], out_sems.at[4 + i * (SLOTS + 1) + SLOTS]
        )
        copy.start()
        outs.append(copy)
    for copy in tops + outs:
        copy.wait()


def body(
    root_frame,
    top_lhat,
    top_dinv,
    mid_lhat,
    mid_dinv,
    leaf_lhat,
    leaf_dinv,
    top_columns,
    mid_columns,
    leaf_columns,
    top_pattern,
    mid_parent,
    leaf_parent,
    mid_pattern,
    leaf_pattern,
    leaf_live,
):
    n = lax.axis_size("leaf")
    cols = top_dinv.shape[1]
    frame = SLOTS * cols
    per = root_frame.shape[1] // cols
    leaves = leaf_lhat.shape[0]
    pool = per * per + NODES2 * OWN

    def dma(count):
        return pltpu.SemaphoreType.DMA((count,))

    def part_sems(group, line, side):
        return [dma(group // 2), dma(1), dma(line), dma(side), dma(1), dma(1)]

    sems = part_sems(n, n // 2 + 2, 1) + part_sems(GROUP2, GROUP2 // 2 + 2, 1)
    for _ in range(2):
        sems += part_sems(GROUP2, GROUP2 // 2 + 2, GROUP2 // GROUP1)
    for _ in range(2 + SLOTS):
        sems += part_sems(GROUP1, 1, 1)
    vmem = pl.BlockSpec(memory_space=pltpu.VMEM)
    hbm = pl.BlockSpec(memory_space=pltpu.HBM)
    shape = jax.ShapeDtypeStruct
    moved = (top_columns, top_pattern, root_frame, top_lhat, top_dinv, mid_lhat[0], mid_dinv[0])
    pool_h, pool_l, top_coup, top_diag, ml_all, md_all = pl.pallas_call(
        functools.partial(gather_kernel, n),
        out_shape=[
            shape((pool, cols, cols), bf16),
            shape((pool, cols, cols), bf16),
            shape(top_lhat.shape, f32),
            shape(top_dinv.shape, f32),
            shape((GROUP1, frame, cols), f32),
            shape((GROUP1, cols, cols), f32),
        ],
        in_specs=[hbm] * 7,
        out_specs=[vmem] * 6,
        scratch_shapes=[
            pltpu.VMEM((per * cols, per * cols), f32),
            pltpu.VMEM((NODES2 * frame, cols), f32),
            pltpu.VMEM((NODES2 * cols, cols), f32),
            pltpu.VMEM((NODES2 * frame, cols), f32),
            pltpu.VMEM((NODES2 * cols, cols), f32),
            pltpu.VMEM((NODES2, 3 * frame, cols), bf16),
            pltpu.SMEM(top_columns.shape, jnp.int32),
            pltpu.SMEM(top_pattern.shape, jnp.int32),
            dma(2),
        ]
        + sems,
        compiler_params=pltpu.CompilerParams(
            collective_id=0, has_side_effects=True, vmem_limit_bytes=20 * 1024 * 1024
        ),
    )(*[in_hbm(x) for x in moved])
    small = (
        mid_columns,
        leaf_columns,
        top_pattern,
        mid_parent,
        leaf_parent,
        mid_pattern.T,
        leaf_pattern.T,
        leaf_live,
    )
    outs = pl.pallas_call(
        functools.partial(tree_kernel, per),
        out_shape=[
            shape(top_dinv.shape, f32),
            shape(top_lhat.shape, f32),
            shape(mid_dinv.shape[1:], f32),
            shape(mid_lhat.shape[1:], f32),
            shape(leaf_dinv.shape, f32),
            shape(leaf_lhat.shape, f32),
        ],
        in_specs=[hbm] * 8 + [vmem] * 6 + [hbm] * 2,
        out_specs=[hbm] * 6,
        scratch_shapes=[
            pltpu.VMEM((leaves + 1, OWN, cols, cols), bf16),
            pltpu.VMEM((leaves + 1, OWN, cols, cols), bf16),
            pltpu.VMEM((leaves + 1, 3 * frame, cols), bf16),
            pltpu.VMEM(leaf_lhat.shape, f32),
            pltpu.VMEM(leaf_dinv.shape, f32),
            pltpu.VMEM((frame, cols), f32),
            pltpu.VMEM((cols, cols), f32),
            pltpu.VMEM(leaf_lhat.shape, f32),
            pltpu.VMEM(leaf_dinv.shape, f32),
        ]
        + [pltpu.SMEM(x.shape, jnp.int32) for x in small]
        + [dma(len(small) + 2), dma(4 + leaves * (SLOTS + 1))],
        compiler_params=pltpu.CompilerParams(vmem_limit_bytes=24 * 1024 * 1024),
    )(
        *[in_hbm(x) for x in small],
        pool_h,
        pool_l,
        top_coup,
        top_diag,
        ml_all,
        md_all,
        in_hbm(leaf_lhat),
        in_hbm(leaf_dinv),
    )
    return (outs[0], outs[1], outs[2][None], outs[3][None], outs[4], outs[5])


def solution(mesh):
    rows = P(("pole", "leaf"), None)
    stacks = P(("pole", "leaf"), None, None)
    in_specs = (rows,) * 3 + (stacks,) * 4 + (P(),) * 9
    out_specs = (rows,) * 2 + (stacks,) * 4
    return jax.shard_map(body, mesh=mesh, in_specs=in_specs, out_specs=out_specs, check_vma=False)
```

```python
import functools

import jax
import jax.numpy as jnp
from jax import lax
from jax.experimental import pallas as pl
from jax.experimental.pallas import tpu as pltpu
from jax.sharding import PartitionSpec as P

SLOTS = 3
GROUP2 = 16
NODES2 = 2
GROUP1 = 4
TILE = 128
OWN = 2 * SLOTS + 1

MESH = pl.DeviceIdType.MESH
f32 = jnp.float32
bf16 = jnp.bfloat16


def split(value):
    high = value.astype(bf16)
    low = (value - high.astype(f32)).astype(bf16)
    return high, low


def in_hbm(x):
    return pltpu.with_memory_space_constraint(x, pltpu.HBM)


def root_windows(tiles):
    if tiles == 8:
        return [(0, 8), (1, 7), (2, 6), (3, 6), (4, 6), (5, 6), (2, 7), (1, 8)]
    return [(r, tiles) for r in range(tiles)]


def half_windows(tiles):
    return [(r, tiles) for r in range(tiles)]


class Part:
    def __init__(self, own, place, group, sems, me, total, rows=0, windows=None):
        self.own, self.place, self.group, self.total = own, place, group, total
        self.recv, self.recv_core, self.line, self.side, self.core, self.local = sems
        self.base = me - lax.rem(me, group)
        self.rows, self.windows = rows, windows
        self.me = me

    def cases(self, device, act):
        if self.windows is None:
            act(None)
            return
        row = lax.rem(lax.div((device - self.base) * self.rows, TILE), len(self.windows))
        for i, window in enumerate(self.windows):
            pl.when(row == i)(functools.partial(act, window))

    def view(self, ref, window):
        if window is None:
            return ref
        return ref.at[:, window[0] * TILE : window[1] * TILE]

    def copy(self, device, window, target, send, recv, own=False):
        dst = self.view(self.place(device - self.base), window)
        return pltpu.make_async_remote_copy(
            src_ref=self.view(self.own, window) if own else dst,
            dst_ref=dst,
            send_sem=send,
            recv_sem=recv,
            device_id={"leaf": target},
            device_id_type=MESH,
        )

    def slot(self, device):
        return lax.div(device - self.base, 2)

    def to_line(self, device, window, target, way, own):
        slot = self.slot(device)
        index = slot
        if isinstance(way, int) and way == 1:
            index = self.group // 2 + lax.rem(slot, 2)
        return self.copy(
            device, window, target, self.line.at[index], self.recv.at[slot], own
        )

    def to_side(self, device, window, target, own):
        index = lax.div(device - self.base, GROUP1) if self.side.shape[0] > 1 else 0
        slot = self.slot(device)
        return self.copy(device, window, target, self.side.at[index], self.recv.at[slot], own)

    def to_core(self, device, window, target, own):
        return self.copy(device, window, target, self.core.at[0], self.recv_core.at[0], own)

    def arrived(self, device, window):
        self.to_line(device, window, self.me, 0, False).wait_recv()

    def all_core(self):
        return pltpu.make_async_remote_copy(
            src_ref=self.total,
            dst_ref=self.total,
            send_sem=self.core.at[0],
            recv_sem=self.recv_core.at[0],
            device_id={"leaf": self.me},
            device_id_type=MESH,
        )

    def keep(self, window):
        return pltpu.make_async_copy(
            self.view(self.own, window),
            self.view(self.place(self.me - self.base), window),
            self.local.at[0],
        )


def start(copy):
    copy.start()


def wait_send(copy):
    copy.wait_send()


def dinv_of(block, cols):
    half = cols // 2
    top = block[:half]
    low = jnp.concatenate([top[:, half:].T, block[half:, half:]], axis=1)
    return jnp.concatenate([top, low], axis=0)


def solve_all(cols, lcats, jobs, after=None):
    row_ids = lax.broadcasted_iota(jnp.int32, (cols, cols), 0)
    lane_ids = lax.broadcasted_iota(jnp.int32, (cols, cols), 1)
    for i, (blocks, lhat, dinv, used, put_coup, put_diag, put) in enumerate(jobs):
        for r in range(SLOTS):
            high, low = split(jnp.where(lane_ids < used, lhat(r), 0.0))
            for part, value in enumerate((high, low, high)):
                first = (3 * r + part) * cols
                lcats[i, first : first + cols] = value
    turned = [[] for _ in jobs]
    for r in range(SLOTS):
        for i, (blocks, lhat, dinv, used, put_coup, put_diag, put) in enumerate(jobs):
            parts = []
            for k in range(SLOTS):
                high, low = blocks(r, k)
                parts += [high, high, low]
            wide = jnp.concatenate(parts, axis=1)
            coup = -jnp.dot(wide, lcats[i], preferred_element_type=f32)
            put_coup(r, coup)
            high, low = split(coup)
            high_t, low_t = high.T, low.T
            if put is not None:
                put(1 + r, high, low)
                put(1 + SLOTS + r, high_t, low_t)
            turned[i] += [high_t, high_t, low_t]
        if after is not None:
            after(r)
    for i, (blocks, lhat, dinv, used, put_coup, put_diag, put) in enumerate(jobs):
        wide = jnp.concatenate(turned[i], axis=1)
        product = jnp.dot(wide, lcats[i], preferred_element_type=f32)
        keep = (lane_ids < used) & (row_ids < used)
        diag = jnp.where(keep, dinv(), 0.0) - product
        put_diag(diag)
        if put is not None:
            put(0, *split(diag))


def gather_kernel(
    n,
    columns_in,
    pattern_in,
    root_in,
    tl_in,
    td_in,
    ml_in,
    md_in,
    pool_h,
    pool_l,
    top_coup_out,
    top_diag_out,
    ml_all,
    md_all,
    root_all,
    tl_all,
    td_all,
    top_c,
    top_d,
    lcats,
    columns,
    pattern,
    small_sems,
    *sems,
):
    me = lax.axis_index("leaf")
    core = lax.rem(me, 2)
    side = lax.rem(lax.div(me, 2), 2)
    cpeer = me + 1 - 2 * core
    xpeer = me + 2 - 4 * side
    other = cpeer + xpeer - me
    cols = td_in.shape[1]
    frame = SLOTS * cols
    half = cols // 2
    per = root_in.shape[1] // cols

    def rows_of(ref, rows, first, count):
        return lambda slot: ref.at[pl.ds(pl.multiple_of(slot * rows + first, 8), count)]

    def next_sems():
        nonlocal sems
        taken, sems = sems[:6], sems[6:]
        return taken

    def by_rows(own, whole, group, windows=None, first=0, last=None):
        rows, width = own.shape
        count = (rows if last is None else last) - first
        tiles = width // TILE
        widths = [c1 - c0 for c0, c1 in windows] if windows else [tiles]
        half_of = group * count // 2 * sum(widths) // (len(widths) * tiles)
        place = rows_of(whole, rows, first, count)
        own = own.at[pl.ds(first, count)]
        return Part(own, place, group, next_sems(), me, whole.at[0:half_of], rows, windows)

    root = by_rows(root_in, root_all, n, root_windows(per * cols // TILE))
    middle = tl_in.shape[0] // 2 // 8 * 8
    tl = by_rows(tl_in, tl_all, GROUP2, None, 0, middle)
    tl_side = by_rows(tl_in, tl_all, GROUP2, None, middle)
    td = by_rows(td_in, td_all, GROUP2, half_windows(cols // TILE))

    def mid_part(own, whole, *index):
        place = lambda slot: whole.at[(slot,) + index]
        total = whole.at[(slice(0, 2),) + index]
        return Part(own.at[index], place, GROUP1, next_sems(), me, total)

    md0 = mid_part(md_in, md_all, slice(0, half))
    md1 = mid_part(md_in, md_all, slice(half, cols), slice(half, cols))
    mls = [mid_part(ml_in, ml_all, slice(r * cols, (r + 1) * cols)) for r in range(SLOTS)]
    mids = (md0, md1) + tuple(mls)

    line = n // GROUP1
    place = lax.div(me, GROUP1)
    top_line = GROUP2 // GROUP1
    top_place = lax.div(lax.rem(me, GROUP2), GROUP1)
    has_next = (place < line - 1, place > 0)
    top_next = (top_place < top_line - 1, top_place > 0)

    fetches = [
        pltpu.make_async_copy(a, b, small_sems.at[i])
        for i, (a, b) in enumerate([(columns_in, columns), (pattern_in, pattern)])
    ]
    for fetch in fetches:
        fetch.start()

    barrier = pltpu.get_barrier_semaphore()

    def greet(target):
        pl.semaphore_signal(barrier, inc=1, device_id={"leaf": target}, device_id_type=MESH)

    greet(cpeer)
    greet(xpeer)
    pl.when(has_next[0])(lambda: greet(me + GROUP1))
    pl.when(has_next[1])(lambda: greet(me - GROUP1))
    both = (root, tl)
    single = (td, tl_side)
    everything = single + both + mids
    for part in everything:
        part.cases(me, lambda w, part=part: part.keep(w).start())
    peers = 2 + jnp.minimum(place, 1) + jnp.minimum(line - 1 - place, 1)
    pl.semaphore_wait(barrier, peers)

    def along(part, device, window, way, act, own=False):
        up, down = has_next if part.group == n else top_next
        if isinstance(way, int):
            ok, target = (down, me - GROUP1) if way else (up, me + GROUP1)
        else:
            ok, target = jnp.where(way == 0, up, down), me + GROUP1 - 2 * GROUP1 * way
        pl.when(ok)(lambda: act(part.to_line(device, window, target, way, own)))

    def side_to(part, device, window, act, own=False):
        act(part.to_side(device, window, xpeer, own))

    def core_to(part, device, window, act, own=False):
        if act is start:
            act(part.to_core(device, window, cpeer, own))

    def own_moves(part, act, lines=True, side=True, core=True):
        def moves(window):
            if lines:
                along(part, me, window, 0, act, True)
                along(part, me, window, 1, act, True)
            if side:
                side_to(part, me, window, act, True)
            if core:
                core_to(part, me, window, act, True)

        part.cases(me, moves)

    for part in both:
        own_moves(part, start, lines=False, core=False)
    for part in single + both:
        own_moves(part, start, side=False, core=False)
    for part in single + mids[:3]:
        own_moves(part, start, lines=False, core=False)
    for part in everything:
        own_moves(part, start, lines=False, side=False)

    def passed(part, device, way, act, side=False, wait=False):
        def moves(window):
            if wait:
                part.arrived(device, window)
            if way is None:
                along(part, device, window, 0, act)
                along(part, device, window, 1, act)
            else:
                along(part, device, window, way, act)
            if side:
                side_to(part, device, window, act)
            core_to(part, device, window, act)

        part.cases(device, moves)

    for part in both:
        passed(part, xpeer, None, start, wait=True)

    outer = lax.div(2 * place, line)

    last_step = jnp.maximum(top_place, top_line - 1 - top_place)

    def steps(act, wait):
        def step(s, carry):
            def turned(t):
                way = lax.rem(t + 1 + outer, 2)
                shift = (2 * way - 1) * s * GROUP1
                got_top = jnp.where(way == 0, top_place >= s, top_place + s < top_line)
                got_root = jnp.where(way == 0, place >= s, place + s < line)
                return way, shift, got_top, got_root

            def crossing(t, carry):
                way, shift, got_top, _ = turned(t)

                @pl.when(got_top)
                def _():
                    for part in single:
                        passed(part, me + shift, way, act, side=True, wait=wait)

                return carry

            lax.fori_loop(0, 2, crossing, 0)
            if wait:
                @pl.when(s == last_step)
                def _():
                    own_moves(mls[2], start, lines=False, core=False)

            def turn(t, carry):
                way, shift, got_top, got_root = turned(t)

                def one(i, carry):
                    device = jnp.where(i == 0, me, xpeer) + shift

                    @pl.when(got_root)
                    def _():
                        passed(root, device, way, act, wait=wait)

                    @pl.when(got_top)
                    def _():
                        passed(tl, device, way, act, wait=wait)

                    return carry

                lax.fori_loop(0, 2, one, 0)
                return carry

            lax.fori_loop(0, 2, turn, 0)
            if wait:
                @pl.when(s == 1)
                def _():
                    own_moves(mls[1], start, lines=False, core=False)

            return carry

        lax.fori_loop(1, line, step, 0)

    steps(start, True)

    def crossed(part, device, act, wait):
        def moves(window):
            if wait:
                part.arrived(device, window)
            core_to(part, device, window, act)

        part.cases(device, moves)

    def tops_crossed(act, wait):
        for q in range(top_line):
            for part in single:
                crossed(part, part.base + q * GROUP1 + lax.rem(xpeer, GROUP1), act, wait)

    tops_crossed(start, True)
    for part in mids[:4]:
        crossed(part, xpeer, start, True)

    def from_core(part):
        part.all_core().wait_recv()
        part.cases(me, lambda w: part.keep(w).wait())

    from_core(root)
    tiles = cols // TILE
    windows = root.windows
    for r, (c0, c1) in enumerate(windows):
        for c in range(c0, c1):
            value = root_all[r * TILE : (r + 1) * TILE, c * TILE : (c + 1) * TILE]
            for a, b, tile in ((r, c, value), (c, r, value.T))[: 1 if r == c else 2]:
                high, low = split(tile)
                index = (a // tiles) * per + b // tiles
                rows = slice(a % tiles * TILE, (a % tiles + 1) * TILE)
                lanes = slice(b % tiles * TILE, (b % tiles + 1) * TILE)
                pool_h[index, rows, lanes] = high
                pool_l[index, rows, lanes] = low
    for fetch in fetches:
        fetch.wait()
    for part in single + (tl,):
        from_core(part)

    top_base = lax.div(me, GROUP2) * NODES2
    roots = per * per

    def top_job(q):
        chosen = [pattern[top_base + q, k] for k in range(SLOTS)]

        def blocks(r, k):
            index = chosen[r] * per + chosen[k]
            return pool_h[index], pool_l[index]

        def lhat(r):
            return tl_all[q * frame + r * cols : q * frame + (r + 1) * cols]

        def put_coup(r, value):
            top_c[q * frame + r * cols : q * frame + (r + 1) * cols] = value

        def put_diag(value):
            top_d[q * cols : (q + 1) * cols] = value

        def put(which, high, low):
            pool_h[roots + q * OWN + which] = high
            pool_l[roots + q * OWN + which] = low

        def dinv():
            return dinv_of(td_all[q * cols : (q + 1) * cols], cols)

        return blocks, lhat, dinv, columns[top_base + q], put_coup, put_diag, put

    solve_all(cols, lcats, [top_job(q) for q in range(NODES2)])
    member = lax.rem(me, GROUP2)
    rows = top_coup_out.shape[0]
    top_coup_out[...] = top_c[pl.ds(pl.multiple_of(member * rows, 8), rows)]
    rows = top_diag_out.shape[0]
    top_diag_out[...] = top_d[pl.ds(pl.multiple_of(member * rows, 8), rows)]

    crossed(mls[2], xpeer, start, True)
    for part in both:
        own_moves(part, wait_send)
        passed(part, xpeer, None, wait_send)
    for part in single:
        own_moves(part, wait_send)
    for part in mids:
        own_moves(part, wait_send, lines=False)
    steps(wait_send, False)
    for part in mids:
        from_core(part)
    for part in everything:
        part.all_core().wait_send()


def tree_kernel(per, *refs):
    small_in, refs = refs[:8], refs[8:]
    pool_h, pool_l, top_coup, top_diag, ml_all, md_all, leaf_lhat_in, leaf_dinv_in = refs[:8]
    top_diag_out, top_coup_out, mid_diag_out, mid_coup_out, leaf_diag_out, leaf_coup_out = refs[8:14]
    e1h, e1l, lcats, leaf_lhat, leaf_dinv, mid_c, mid_d, leaf_c, leaf_d = refs[14:23]
    small = refs[23:31]
    in_sems, out_sems = refs[31:]
    (
        mid_columns,
        leaf_columns,
        top_pattern,
        mid_parent,
        leaf_parent,
        mid_pattern,
        leaf_pattern,
        leaf_live,
    ) = small
    fetched = list(zip(small_in + (leaf_lhat_in, leaf_dinv_in), small + (leaf_lhat, leaf_dinv)))
    fetches = [pltpu.make_async_copy(a, b, in_sems.at[i]) for i, (a, b) in enumerate(fetched)]
    for fetch in fetches:
        fetch.start()
    tops = [
        pltpu.make_async_copy(top_coup, top_coup_out, out_sems.at[0]),
        pltpu.make_async_copy(top_diag, top_diag_out, out_sems.at[1]),
    ]
    for copy in tops:
        copy.start()
    me = lax.axis_index("leaf")
    leaves, cols = leaf_dinv.shape[0], leaf_dinv.shape[2]
    roots = per * per
    top_base = lax.div(me, GROUP2) * NODES2
    mid_base = lax.div(me, GROUP1) * GROUP1
    mine = lax.rem(me, GROUP1)
    for fetch in fetches[:-2]:
        fetch.wait()
    live = leaf_live[me]

    def pool_index(node, u, v):
        parent = mid_parent[node] - top_base
        a = mid_pattern[u, node]
        b = mid_pattern[v, node]
        base = roots + parent * OWN
        near = base + jnp.where(b == 0, a, SLOTS + b)
        far_a = top_pattern[top_base + parent, jnp.maximum(a - 1, 0)]
        far_b = top_pattern[top_base + parent, jnp.maximum(b - 1, 0)]
        return jnp.where((a == 0) | (b == 0), near, far_a * per + far_b)

    parents = [leaf_parent[me * leaves + i] - mid_base for i in range(leaves)]

    def mid_job(k):
        local = parents[k - 1] if k else mine
        node = mid_base + local

        def blocks(r, c):
            index = pool_index(node, r, c)
            return pool_h[index], pool_l[index]

        def lhat(r):
            return ml_all[local, r * cols : (r + 1) * cols]

        def put_coup(r, value):
            if k == 0:
                mid_c[r * cols : (r + 1) * cols] = value

        def put_diag(value):
            if k == 0:
                mid_d[...] = value

        def put(which, high, low):
            e1h[k, which] = high
            e1l[k, which] = low

        def dinv():
            return dinv_of(md_all[local], cols)

        return blocks, lhat, dinv, mid_columns[node], put_coup, put_diag, put

    solve_all(cols, lcats, [mid_job(k) for k in range(leaves + 1)])
    outs = [
        pltpu.make_async_copy(mid_c, mid_coup_out, out_sems.at[2]),
        pltpu.make_async_copy(mid_d, mid_diag_out, out_sems.at[3]),
    ]
    for copy in outs:
        copy.start()
    for fetch in fetches[-2:]:
        fetch.wait()

    def leaf_job(i):
        node = me * leaves + i
        above = mid_base + parents[i]
        alive = jnp.full((cols, cols), i, jnp.int32) < live

        def blocks(r, c):
            if r == 0 or c == 0:
                if r == 0:
                    which = leaf_pattern[c, node] + SLOTS if c else 0
                else:
                    which = leaf_pattern[r, node]
                return e1h[i + 1, which], e1l[i + 1, which]
            index = pool_index(above, leaf_pattern[r, node] - 1, leaf_pattern[c, node] - 1)
            return pool_h[index], pool_l[index]

        def lhat(r):
            return leaf_lhat[i, r * cols : (r + 1) * cols]

        def put_coup(r, value):
            leaf_c[i, r * cols : (r + 1) * cols] = jnp.where(alive, value, 0.0)

        def put_diag(value):
            leaf_d[i] = jnp.where(alive, value, 0.0)

        def dinv():
            return leaf_dinv[i]

        return blocks, lhat, dinv, leaf_columns[node], put_coup, put_diag, None

    def leaf_rows(r):
        for i in range(leaves):
            rows = pl.ds(r * cols, cols)
            copy = pltpu.make_async_copy(
                leaf_c.at[i, rows],
                leaf_coup_out.at[i, rows],
                out_sems.at[4 + i * (SLOTS + 1) + r],
            )
            copy.start()
            outs.append(copy)

    def after(r):
        if r:
            leaf_rows(r - 1)

    solve_all(cols, lcats, [leaf_job(i) for i in range(leaves)], after)
    leaf_rows(SLOTS - 1)
    for i in range(leaves):
        copy = pltpu.make_async_copy(
            leaf_d.at[i], leaf_diag_out.at[i], out_sems.at[4 + i * (SLOTS + 1) + SLOTS]
        )
        copy.start()
        outs.append(copy)
    for copy in tops + outs:
        copy.wait()


def body(
    root_frame,
    top_lhat,
    top_dinv,
    mid_lhat,
    mid_dinv,
    leaf_lhat,
    leaf_dinv,
    top_columns,
    mid_columns,
    leaf_columns,
    top_pattern,
    mid_parent,
    leaf_parent,
    mid_pattern,
    leaf_pattern,
    leaf_live,
):
    n = lax.axis_size("leaf")
    cols = top_dinv.shape[1]
    frame = SLOTS * cols
    per = root_frame.shape[1] // cols
    leaves = leaf_lhat.shape[0]
    pool = per * per + NODES2 * OWN

    def dma(count):
        return pltpu.SemaphoreType.DMA((count,))

    def part_sems(group, line, side):
        return [dma(group // 2), dma(1), dma(line), dma(side), dma(1), dma(1)]

    sems = part_sems(n, n // 2 + 2, 1) + part_sems(GROUP2, GROUP2 // 2 + 2, 1)
    for _ in range(2):
        sems += part_sems(GROUP2, GROUP2 // 2 + 2, GROUP2 // GROUP1)
    for _ in range(2 + SLOTS):
        sems += part_sems(GROUP1, 1, 1)
    vmem = pl.BlockSpec(memory_space=pltpu.VMEM)
    hbm = pl.BlockSpec(memory_space=pltpu.HBM)
    shape = jax.ShapeDtypeStruct
    moved = (top_columns, top_pattern, root_frame, top_lhat, top_dinv, mid_lhat[0], mid_dinv[0])
    pool_h, pool_l, top_coup, top_diag, ml_all, md_all = pl.pallas_call(
        functools.partial(gather_kernel, n),
        out_shape=[
            shape((pool, cols, cols), bf16),
            shape((pool, cols, cols), bf16),
            shape(top_lhat.shape, f32),
            shape(top_dinv.shape, f32),
            shape((GROUP1, frame, cols), f32),
            shape((GROUP1, cols, cols), f32),
        ],
        in_specs=[hbm] * 7,
        out_specs=[vmem] * 6,
        scratch_shapes=[
            pltpu.VMEM((per * cols, per * cols), f32),
            pltpu.VMEM((NODES2 * frame, cols), f32),
            pltpu.VMEM((NODES2 * cols, cols), f32),
            pltpu.VMEM((NODES2 * frame, cols), f32),
            pltpu.VMEM((NODES2 * cols, cols), f32),
            pltpu.VMEM((NODES2, 3 * frame, cols), bf16),
            pltpu.SMEM(top_columns.shape, jnp.int32),
            pltpu.SMEM(top_pattern.shape, jnp.int32),
            dma(2),
        ]
        + sems,
        compiler_params=pltpu.CompilerParams(
            collective_id=0, has_side_effects=True, vmem_limit_bytes=20 * 1024 * 1024
        ),
    )(*[in_hbm(x) for x in moved])
    small = (
        mid_columns,
        leaf_columns,
        top_pattern,
        mid_parent,
        leaf_parent,
        mid_pattern.T,
        leaf_pattern.T,
        leaf_live,
    )
    outs = pl.pallas_call(
        functools.partial(tree_kernel, per),
        out_shape=[
            shape(top_dinv.shape, f32),
            shape(top_lhat.shape, f32),
            shape(mid_dinv.shape[1:], f32),
            shape(mid_lhat.shape[1:], f32),
            shape(leaf_dinv.shape, f32),
            shape(leaf_lhat.shape, f32),
        ],
        in_specs=[hbm] * 8 + [vmem] * 6 + [hbm] * 2,
        out_specs=[hbm] * 6,
        scratch_shapes=[
            pltpu.VMEM((leaves + 1, OWN, cols, cols), bf16),
            pltpu.VMEM((leaves + 1, OWN, cols, cols), bf16),
            pltpu.VMEM((leaves + 1, 3 * frame, cols), bf16),
            pltpu.VMEM(leaf_lhat.shape, f32),
            pltpu.VMEM(leaf_dinv.shape, f32),
            pltpu.VMEM((frame, cols), f32),
            pltpu.VMEM((cols, cols), f32),
            pltpu.VMEM(leaf_lhat.shape, f32),
            pltpu.VMEM(leaf_dinv.shape, f32),
        ]
        + [pltpu.SMEM(x.shape, jnp.int32) for x in small]
        + [dma(len(small) + 2), dma(4 + leaves * (SLOTS + 1))],
        compiler_params=pltpu.CompilerParams(vmem_limit_bytes=24 * 1024 * 1024),
    )(
        *[in_hbm(x) for x in small],
        pool_h,
        pool_l,
        top_coup,
        top_diag,
        ml_all,
        md_all,
        in_hbm(leaf_lhat),
        in_hbm(leaf_dinv),
    )
    return (outs[0], outs[1], outs[2][None], outs[3][None], outs[4], outs[5])


def solution(mesh):
    rows = P(("pole", "leaf"), None)
    stacks = P(("pole", "leaf"), None, None)
    in_specs = (rows,) * 3 + (stacks,) * 4 + (P(),) * 9
    out_specs = (rows,) * 2 + (stacks,) * 4
    return jax.shard_map(body, mesh=mesh, in_specs=in_specs, out_specs=out_specs, check_vma=False)
```
